32 devices in a mesh: ty: 4 (over y, x), tx: 8 (over z, core).
Axes of the slice: x: 2, y: 2, z: 4, core: 2. Of those that a mesh axis runs over, the one named last changes fastest.
Arguments:
- sky: bfloat16 [2048, 4096], P('ty', 'tx'), may hold values from -6 to 6
- point_count: int32 [4, 8], P('ty', 'tx'), may hold values from 0 to 4, as said below
- point_offset: int32 [4, 8, 4, 2], P('ty', 'tx'), may hold values from 0 to 511
- beam_width: bfloat16 [4, 8, 4], P('ty', 'tx'), may hold values from 128 to 340
- uv_bins: int32 [4, 8, 4, 2, 2], P('ty', 'tx'), may hold values from 0 to 7
- uv_count: int32 [4, 8, 4], P('ty', 'tx'), may hold values from 1 to 2
- uv_weight: bfloat16 [4, 8, 4, 2, 128, 128], P('ty', 'tx'), may hold values from 1 to 8
Outputs:
- curvature: float32 [2048, 4096], P('ty', 'tx')
The draws below stay inside these ranges and needn't reach their ends.
Inputs may be any that keep to these rules, and one draw needn't show every extreme that they name: `point_count`: each tile holds at most 4 pointings, and the tiles of columns 2i and 2i + 1 of one row hold at most 4 together; in every draw some such pair holds exactly 4, all on one of its tiles. `point_offset`: entries of slots at or beyond a tile's count are ignored. `uv_bins`: entries of uv slots at or beyond a pointing's uv_count are ignored.
All inputs are finite; a program needn't handle non-finite values.
Results may differ from the reference program's by a relative error of at most 0.0085.
Values may be sent and summed in bfloat16 or wider, within the bound.
A program may use at most 128 MiB of HBM per device.

```python
import math
import jax
import jax.numpy as jnp
from jax import lax

TILE = 512
UVB = 128
UVSLOT = 2
SLOTS = 4
UVBLK = 8
GRID_Y = 4
GRID_X = 8
SKY_Y = 2048
SKY_X = 4096


def draw_point_count(key, part):
    key_total, key_first, key_where, key_side = jax.random.split(jax.random.fold_in(key, 11), 4)
    pairs = GRID_X // 2
    totals = jax.random.randint(key_total, (GRID_Y, pairs), 2, SLOTS + 1)
    first = jax.random.randint(key_first, (GRID_Y, pairs), 0, totals + 1)
    chosen = jax.random.randint(key_where, (), 0, GRID_Y * pairs)
    side = jax.random.randint(key_side, (), 0, 2)
    flat = jnp.arange(GRID_Y * pairs, dtype=jnp.int32).reshape(GRID_Y, pairs)
    hit = flat == chosen
    totals = jnp.where(hit, SLOTS, totals)
    first = jnp.where(hit, side * SLOTS, first)
    second = totals - first
    return jnp.stack([first, second], axis=-1).reshape(GRID_Y, GRID_X).astype(jnp.int32)


def set_ends(entries, stream_key, smallest, high):
    extent = entries.shape
    spot = [jax.random.randint(jax.random.fold_in(stream_key, axis), (), 0, extent[axis]) for axis in range(len(extent))]
    entries = entries.at[tuple(spot)].set(smallest)
    longest = extent.index(max(extent))
    spot[longest] = (spot[longest] + 1) % extent[longest]
    return entries.at[tuple(spot)].set(high)


def level_of(rng, shape, shards, low, largest):
    level, own = 1.0, jax.random.fold_in(rng, 6)
    for dim, shards_of in shards:
        heights = jnp.exp(jax.random.uniform(jax.random.fold_in(own, dim), (shards_of,), jnp.float32, low / len(shards), largest / len(shards)))
        level = level * jnp.repeat(heights, shape[dim] // shards_of).reshape([-1 if axis == dim else 1 for axis in range(len(shape))])
    return level


def normal_values(rng, extent, scale, limit, cuts=(), kind=jnp.bfloat16):
    values = jax.random.normal(rng, extent, jnp.float32) * scale
    if len(cuts) > 0:
        values = level_of(rng, extent, cuts, -0.22, 0.18) * values
    return jnp.clip(values, min=-limit, max=limit).astype(kind)


def setup_inputs(seed: int = 0) -> dict:
    keys = jax.random.split(jax.random.key(seed), 8)
    sky = normal_values(keys[0], (SKY_Y, SKY_X), 1.0, 6.0, ((0, 4), (1, 8)))
    point_count = draw_point_count(jax.random.fold_in(keys[7], 71), 0)
    point_offset = set_ends(jax.random.randint(keys[2], (GRID_Y, GRID_X, SLOTS, 2), 0, TILE), jax.random.fold_in(keys[2], 1), 0, TILE - 1).astype(jnp.int32)
    beam_width = jnp.clip(jnp.exp(math.log(340.0) - 0.97691535 * jax.random.uniform(keys[3], (GRID_Y, GRID_X, SLOTS), jnp.float32) ** level_of(keys[3], (GRID_Y, GRID_X, SLOTS), ((0, 4), (1, 8)), -0.2, 0.2)), 128.0, 340.0).astype(jnp.bfloat16)
    uv_bins = set_ends(jax.random.randint(keys[4], (GRID_Y, GRID_X, SLOTS, UVSLOT, 2), 0, UVBLK), jax.random.fold_in(keys[4], 1), 0, UVBLK - 1).astype(jnp.int32)
    uv_count = set_ends(jax.random.randint(keys[5], (GRID_Y, GRID_X, SLOTS), 1, UVSLOT + 1), jax.random.fold_in(keys[5], 1), 1, UVSLOT).astype(jnp.int32)
    uv_weight = jnp.clip(jnp.exp(math.log(8.0) - 2.0794415 * jax.random.uniform(keys[6], (GRID_Y, GRID_X, SLOTS, UVSLOT, UVB, UVB), jnp.float32) ** level_of(keys[6], (GRID_Y, GRID_X, SLOTS, UVSLOT, UVB, UVB), ((0, 4), (1, 8)), -0.2, 0.2)), 1.0, 8.0).astype(jnp.bfloat16)
    return {"sky": sky, "point_count": point_count, "point_offset": point_offset, "beam_width": beam_width, "uv_bins": uv_bins, "uv_count": uv_count, "uv_weight": uv_weight}


def dft_tables(blocks, block_size, length):
    rows = blocks[:, None] * block_size + jnp.arange(block_size, dtype=jnp.int32)[None, :]
    pixels = jnp.arange(length, dtype=jnp.int32)
    phase = rows[:, :, None] * pixels[None, None, :] % length
    angle = phase.astype(jnp.float32) * (2.0 * math.pi / length)
    factor = 1.0 / math.sqrt(length)
    return ((jnp.cos(angle) * factor).astype(jnp.bfloat16), (jnp.sin(angle) * factor).astype(jnp.bfloat16))

def beam_map(width, length):
    offset = jnp.arange(length, dtype=jnp.float32) - length // 2
    square = offset * offset
    radius = square[:, None] + square[None, :]
    spread = width.astype(jnp.float32)
    return jnp.exp(-radius / (2.0 * spread * spread))

def pointing_image(beamed, width, uv_pair, used, weight_tiles):
    slots_uv = weight_tiles.shape[0]
    block_size = weight_tiles.shape[1]
    length = beamed.shape[0]
    row_cos, row_sin = dft_tables(uv_pair[:, 0], block_size, length)
    col_cos, col_sin = dft_tables(uv_pair[:, 1], block_size, length)
    row_tables = jnp.stack([row_cos, row_sin], axis=1).reshape(slots_uv * 2 * block_size, length)
    col_tables = jnp.stack([jnp.concatenate([col_cos, col_sin], axis=1), jnp.concatenate([-col_sin, col_cos], axis=1)], axis=1)
    first = jnp.dot(row_tables, beamed, preferred_element_type=jnp.float32).astype(jnp.bfloat16)
    first = first.reshape(slots_uv, 2, block_size, length)
    visible = jnp.einsum('kcin,kcbn->kib', first.astype(jnp.float32), col_tables.astype(jnp.float32))
    used_mask = (jnp.arange(slots_uv, dtype=jnp.int32) < used).astype(jnp.float32)
    weighted = weight_tiles.astype(jnp.float32) * used_mask[:, None, None]
    scaled = (visible * jnp.concatenate([weighted, weighted], axis=2)).astype(jnp.bfloat16)
    spread = jnp.einsum('kib,kcbn->kcin', scaled.astype(jnp.float32), col_tables.astype(jnp.float32))
    spread = spread.astype(jnp.bfloat16).reshape(slots_uv * 2 * block_size, length)
    back = lax.dot_general(row_tables, spread, (((0,), (0,)), ((), ())), preferred_element_type=jnp.float32)
    return (beam_map(width, length) * back).astype(jnp.bfloat16)

def reference(sky, point_count, point_offset, beam_width, uv_bins, uv_count, uv_weight):
    grid_rows, grid_cols = point_count.shape
    slots = point_offset.shape[2]
    tile_size = TILE
    patch_size = 2 * TILE
    padded = jnp.pad(sky, tile_size)
    pairs = grid_cols // 2
    shape = (grid_rows, pairs, slots)
    row_ids = jnp.broadcast_to(jnp.arange(grid_rows, dtype=jnp.int32)[:, None, None], shape)
    pair_ids = jnp.broadcast_to(jnp.arange(pairs, dtype=jnp.int32)[None, :, None], shape)
    combined = jnp.broadcast_to(jnp.arange(slots, dtype=jnp.int32)[None, None, :], shape)
    even_count = point_count[:, 0::2][:, :, None]
    odd_count = point_count[:, 1::2][:, :, None]
    from_odd = (combined >= even_count).astype(jnp.int32)
    columns = 2 * pair_ids + from_odd
    slot_ids = jnp.clip(combined - from_odd * even_count, 0, slots - 1)
    live_ids = combined < even_count + odd_count

    def place(total, item):
        row, col, slot, live = item
        offset = point_offset[row, col, slot]
        top = (row * tile_size + offset[0]).astype(jnp.int32)
        left = (col * tile_size + offset[1]).astype(jnp.int32)
        window = lax.dynamic_slice(padded, (top, left), (patch_size, patch_size))
        width = beam_width[row, col, slot]
        beamed = (beam_map(width, patch_size) * window.astype(jnp.float32)).astype(jnp.bfloat16)
        image = pointing_image(beamed, width, uv_bins[row, col, slot], uv_count[row, col, slot], uv_weight[row, col, slot])
        image = jnp.where(live, image.astype(jnp.float32), jnp.zeros((), jnp.float32))
        current = lax.dynamic_slice(total, (top, left), (patch_size, patch_size))
        return (lax.dynamic_update_slice(total, current + image, (top, left)), None)
    start = jnp.zeros(padded.shape, jnp.float32)
    items = (row_ids.reshape(-1), columns.reshape(-1), slot_ids.reshape(-1), live_ids.reshape(-1))
    total, unused = lax.scan(place, start, items)
    return total[tile_size:-tile_size, tile_size:-tile_size]
```

```python
import functools
import math

import jax
import jax.numpy as jnp
from jax import lax
from jax.experimental import pallas as pl
from jax.experimental.pallas import tpu as pltpu
from jax.sharding import PartitionSpec as P

F32 = jnp.float32
BF16 = jnp.bfloat16
CHUNK = 256


def shifted(value, axis, steps):
    count = lax.axis_size(axis)
    first, last = (max(0, -steps), min(count, count - steps))
    return lax.ppermute(value, axis, [(source, source + steps) for source in range(first, last)])


def full_tables(length):
    index = jnp.arange(length, dtype=jnp.int32)
    phase = index[:, None] * index[None, :] % length
    angle = phase.astype(F32) * (2.0 * math.pi / length)
    factor = 1.0 / math.sqrt(length)
    return (jnp.cos(angle) * factor).astype(BF16), (jnp.sin(angle) * factor).astype(BF16)


def gaussians(start, decay, size, axis):
    shape = (size, 128) if axis == 0 else (8, size)
    index = lax.broadcasted_iota(jnp.int32, shape, axis)

    def value(pixel):
        away = (pixel - start - size).astype(F32)
        return jnp.exp(-(away * away) * decay)

    zero = jnp.zeros(shape, F32)
    low = jnp.where(index >= start, value(index), zero)
    high = jnp.where(index < start, value(index + 2 * size), zero)
    return low, value(index + size), high


def wide(column, width):
    return jnp.concatenate([column] * (width // 128), axis=1)


def beams(p, off_ref, decay_ref, gy_ref, gx_ref, size):
    decay = decay_ref[p]
    for part, values in enumerate(gaussians(off_ref[p, 0], decay, size, 0)):
        gy_ref[part] = values
    for part, values in enumerate(gaussians(off_ref[p, 1], decay, size, 1)):
        gx_ref[part] = values


def row_tables(p, bins_ref, which, cos_ref, sin_ref, rows_ref, block, slots_uv):
    for k in range(slots_uv):
        at = pl.ds(pl.multiple_of(bins_ref[p, 2 * k + which] * block, block), block)
        rows_ref[(2 * k) * block : (2 * k + 1) * block, :] = cos_ref[at, :]
        rows_ref[(2 * k + 1) * block : (2 * k + 2) * block, :] = sin_ref[at, :]


def flipped_tables(p, bins_ref, cos_ref, sin_ref, flip_ref, block, slots_uv):
    for k in range(slots_uv):
        at = pl.ds(pl.multiple_of(bins_ref[p, 2 * k] * block, block), block)
        flip_ref[:, (2 * k) * block : (2 * k + 1) * block] = cos_ref[:, at]
        flip_ref[:, (2 * k + 1) * block : (2 * k + 2) * block] = sin_ref[:, at]


def early_kernel(
    count_ref, off_ref, bins_ref, decay_ref, cos_ref, sin_ref, up_ref, own_ref, down_ref,
    first_ref, gy_ref, gx_ref, rows_ref, beamed_ref,
):
    size = own_ref.shape[0]
    block = rows_ref.shape[0] // bins_ref.shape[1]
    slots_uv = bins_ref.shape[1] // 2

    def step(p, carry):
        beams(p, off_ref, decay_ref, gy_ref, gx_ref, size)
        row_tables(p, bins_ref, 0, cos_ref, sin_ref, rows_ref, block, slots_uv)
        for at in range(0, size, CHUNK):
            cols = slice(at, at + CHUNK)
            gx = gx_ref[1, 0:1, cols]
            top = wide(gy_ref[0], CHUNK) * up_ref[:, cols].astype(F32)
            top = top + wide(gy_ref[2], CHUNK) * down_ref[:, cols].astype(F32)
            beamed_ref[:size, cols] = (gx * top).astype(BF16)
            low = wide(gy_ref[1], CHUNK) * own_ref[:, cols].astype(F32)
            beamed_ref[size:, cols] = (gx * low).astype(BF16)
        for at in range(0, size, CHUNK):
            cols = slice(at, at + CHUNK)
            first_ref[p, :, cols] = jnp.dot(
                rows_ref[...], beamed_ref[:, cols], preferred_element_type=F32
            ).astype(BF16)
        return carry

    lax.fori_loop(0, count_ref[0], step, 0)


def middle_kernel(
    count_ref, off_ref, bins_ref, used_ref, decay_ref, cos_ref, sin_ref, weight_ref, early_ref,
    ul_ref, l_ref, dl_ref, ur_ref, r_ref, dr_ref,
    oul_ref, ol_ref, odl_ref, our_ref, or_ref, odr_ref, late_ref,
    gy_ref, gx_ref, rows_ref, cols_ref, flip_ref, beamed_ref, first_ref, spread_ref, acc_ref,
):
    size = l_ref.shape[0]
    block = rows_ref.shape[0] // bins_ref.shape[1]
    slots_uv = bins_ref.shape[1] // 2
    pair = 2 * block
    acc_ref[...] = jnp.zeros_like(acc_ref)

    def step(p, carry):
        beams(p, off_ref, decay_ref, gy_ref, gx_ref, size)
        row_tables(p, bins_ref, 0, cos_ref, sin_ref, rows_ref, block, slots_uv)
        row_tables(p, bins_ref, 1, cos_ref, sin_ref, cols_ref, block, slots_uv)
        flipped_tables(p, bins_ref, cos_ref, sin_ref, flip_ref, block, slots_uv)
        for at in range(0, size, CHUNK):
            cols = slice(at, at + CHUNK)
            gl = gx_ref[0, 0:1, cols]
            gr = gx_ref[2, 0:1, cols]
            gu = wide(gy_ref[0], CHUNK)
            gd = wide(gy_ref[2], CHUNK)
            left = gu * ul_ref[:, cols].astype(F32) + gd * dl_ref[:, cols].astype(F32)
            right = gu * ur_ref[:, cols].astype(F32) + gd * dr_ref[:, cols].astype(F32)
            beamed_ref[:size, cols] = (gl * left + gr * right).astype(BF16)
            low = gl * l_ref[:, cols].astype(F32) + gr * r_ref[:, cols].astype(F32)
            beamed_ref[size:, cols] = (wide(gy_ref[1], CHUNK) * low).astype(BF16)
        first_ref[:, size:] = early_ref[p]
        for at in range(0, size, CHUNK):
            cols = slice(at, at + CHUNK)
            first_ref[:, cols] = jnp.dot(
                rows_ref[...], beamed_ref[:, cols], preferred_element_type=F32
            ).astype(BF16)
        for k in range(slots_uv):
            rows = slice(k * pair, (k + 1) * pair)
            table = cols_ref[rows, :]
            both = lax.dot_general(
                first_ref[rows, :], table, (((1,), (1,)), ((), ())), preferred_element_type=F32
            )
            used = jnp.where(k < used_ref[p], 1.0, 0.0).astype(F32)
            weight = weight_ref[p, k].astype(F32) * used
            real = ((both[:block, :block] - both[block:, block:]) * weight).astype(BF16)
            turned = ((both[:block, block:] + both[block:, :block]) * weight).astype(BF16)
            scaled = jnp.concatenate(
                [
                    jnp.concatenate([real, turned], axis=1),
                    jnp.concatenate([turned, -real], axis=1),
                ],
                axis=0,
            )
            spread_ref[rows, :] = jnp.dot(scaled, table, preferred_element_type=F32).astype(BF16)
        late_ref[p] = spread_ref[:, size:]
        for at in range(0, size, CHUNK):
            cols = slice(at, at + CHUNK)
            gl = gx_ref[0, 0:1, cols]
            gr = gx_ref[2, 0:1, cols]
            top = jnp.dot(flip_ref[:size, :], spread_ref[:, cols], preferred_element_type=F32)
            up = wide(gy_ref[0], CHUNK) * top
            down = wide(gy_ref[2], CHUNK) * top
            acc_ref[0, :, cols] += gl * up
            acc_ref[2, :, cols] += gl * down
            acc_ref[3, :, cols] += gr * up
            acc_ref[5, :, cols] += gr * down
            low = jnp.dot(flip_ref[size:, :], spread_ref[:, cols], preferred_element_type=F32)
            low = wide(gy_ref[1], CHUNK) * low
            acc_ref[1, :, cols] += gl * low
            acc_ref[4, :, cols] += gr * low
        return carry

    lax.fori_loop(0, count_ref[0], step, 0)
    for part, out_ref in enumerate((oul_ref, ol_ref, odl_ref, our_ref, or_ref, odr_ref)):
        out_ref[...] = acc_ref[part].astype(BF16)


def late_kernel(
    count_ref, off_ref, bins_ref, decay_ref, cos_ref, sin_ref, late_ref,
    up_ref, own_ref, down_ref, gy_ref, gx_ref, flip_ref,
):
    size = own_ref.shape[0]
    block = flip_ref.shape[1] // bins_ref.shape[1]
    slots_uv = bins_ref.shape[1] // 2
    for out_ref in (up_ref, own_ref, down_ref):
        out_ref[...] = jnp.zeros_like(out_ref)

    def step(p, carry):
        beams(p, off_ref, decay_ref, gy_ref, gx_ref, size)
        flipped_tables(p, bins_ref, cos_ref, sin_ref, flip_ref, block, slots_uv)
        for at in range(0, size, CHUNK):
            cols = slice(at, at + CHUNK)
            gx = gx_ref[1, 0:1, cols]
            part = late_ref[p, :, cols]
            top = gx * jnp.dot(flip_ref[:size, :], part, preferred_element_type=F32)
            up_ref[:, cols] += wide(gy_ref[0], CHUNK) * top
            down_ref[:, cols] += wide(gy_ref[2], CHUNK) * top
            low = gx * jnp.dot(flip_ref[size:, :], part, preferred_element_type=F32)
            own_ref[:, cols] += wide(gy_ref[1], CHUNK) * low
        return carry

    lax.fori_loop(0, count_ref[0], step, 0)


def local_call(kernel, scalars, vectors, outs, scratch, flops):
    return pl.pallas_call(
        kernel,
        out_shape=outs,
        in_specs=[pl.BlockSpec(memory_space=pltpu.SMEM)] * len(scalars)
        + [pl.BlockSpec(memory_space=pltpu.VMEM)] * len(vectors),
        out_specs=jax.tree.map(lambda _: pl.BlockSpec(memory_space=pltpu.VMEM), outs),
        scratch_shapes=scratch,
        compiler_params=pltpu.CompilerParams(vmem_limit_bytes=56 * 1024 * 1024),
        cost_estimate=pl.CostEstimate(flops=flops, bytes_accessed=8 << 20, transcendentals=0),
    )(*scalars, *vectors)


def shards(sky, point_count, point_offset, beam_width, uv_bins, uv_count, uv_weight):
    size = sky.shape[0]
    length = 2 * size
    slots, slots_uv, block = uv_weight.shape[2], uv_weight.shape[3], uv_weight.shape[4]
    depth = 2 * slots_uv * block
    up = shifted(sky, "ty", 1)
    down = shifted(sky, "ty", -1)
    left = shifted(sky, "tx", 1)
    right = shifted(sky, "tx", -1)
    up_left = shifted(up, "tx", 1)
    up_right = shifted(up, "tx", -1)
    down_left = shifted(down, "tx", 1)
    down_right = shifted(down, "tx", -1)

    cos, sin = full_tables(length)
    count = point_count.reshape(1)
    offset = point_offset.reshape(slots, 2)
    bins = jnp.clip(uv_bins.reshape(slots, 2 * slots_uv), 0, length // block - 1)
    used = uv_count.reshape(slots)
    width = beam_width.reshape(slots).astype(F32)
    decay = 1.0 / (2.0 * width * width)
    weight = uv_weight.reshape(slots, slots_uv, block, block)

    gy = pltpu.VMEM((3, size, 128), F32)
    gx = pltpu.VMEM((3, 8, size), F32)
    rows = pltpu.VMEM((depth, length), BF16)
    flip = pltpu.VMEM((length, depth), BF16)
    beamed = pltpu.VMEM((length, size), BF16)
    half = jax.ShapeDtypeStruct((slots, depth, size), BF16)
    sent = jax.ShapeDtypeStruct((size, size), BF16)
    kept = jax.ShapeDtypeStruct((size, size), F32)
    flops = 2 * slots * depth * length * size

    early = local_call(
        early_kernel,
        (count, offset, bins, decay),
        (cos, sin, up, sky, down),
        half,
        [gy, gx, rows, beamed],
        flops,
    )
    to_ul, to_l, to_dl, to_ur, to_r, to_dr, late = local_call(
        middle_kernel,
        (count, offset, bins, used, decay),
        (cos, sin, weight, early, up_left, left, down_left, up_right, right, down_right),
        (sent,) * 6 + (half,),
        [
            gy, gx, rows, rows, flip, beamed,
            pltpu.VMEM((depth, length), BF16),
            pltpu.VMEM((depth, length), BF16),
            pltpu.VMEM((6, size, size), F32),
        ],
        3 * flops,
    )
    from_ul = shifted(to_ur, "tx", 1)
    from_ur = shifted(to_ul, "tx", -1)
    from_dl = shifted(to_dr, "tx", 1)
    from_dr = shifted(to_dl, "tx", -1)
    from_l = shifted(to_r, "tx", 1)
    from_r = shifted(to_l, "tx", -1)
    to_up, own, to_down = local_call(
        late_kernel,
        (count, offset, bins, decay),
        (cos, sin, late),
        (kept,) * 3,
        [gy, gx, flip],
        flops,
    )
    to_up = (to_up + from_ul.astype(F32) + from_ur.astype(F32)).astype(BF16)
    to_down = (to_down + from_dl.astype(F32) + from_dr.astype(F32)).astype(BF16)
    from_down = shifted(to_up, "ty", -1)
    from_up = shifted(to_down, "ty", 1)
    result = own + from_l.astype(F32) + from_r.astype(F32)
    return result + from_down.astype(F32) + from_up.astype(F32)


def solution(mesh):
    in_specs = (
        P("ty", "tx"),
        P("ty", "tx"),
        P("ty", "tx", None, None),
        P("ty", "tx", None),
        P("ty", "tx", None, None, None),
        P("ty", "tx", None),
        P("ty", "tx", None, None, None, None),
    )
    out_specs = P("ty", "tx")
    return jax.shard_map(shards, mesh=mesh, in_specs=in_specs, out_specs=out_specs, check_vma=False)
```

```python
import functools
import math

import jax
import jax.numpy as jnp
from jax import lax
from jax.experimental import pallas as pl
from jax.experimental.pallas import tpu as pltpu
from jax.sharding import PartitionSpec as P

F32 = jnp.float32
BF16 = jnp.bfloat16
CHUNK = 256
BANDS = 2
FINE = 32
MESH = pl.DeviceIdType.MESH


def small_tables(length, fine):
    pixels = jnp.arange(length, dtype=jnp.int32)
    rows = jnp.concatenate(
        [jnp.arange(fine, dtype=jnp.int32), fine * jnp.arange(length // fine, dtype=jnp.int32)]
    )
    phase = rows[:, None] * pixels[None, :] % length
    angle = phase.astype(F32) * (2.0 * math.pi / length)
    scale = jnp.where(jnp.arange(rows.shape[0]) < fine, 1.0 / math.sqrt(length), 1.0)[:, None]
    return jnp.cos(angle) * scale, jnp.sin(angle) * scale


def gaussians(start, decay, size, axis):
    shape = (size, 128) if axis == 0 else (8, size)
    index = lax.broadcasted_iota(jnp.int32, shape, axis)

    def value(pixel):
        away = (pixel - start - size).astype(F32)
        return jnp.exp(-(away * away) * decay)

    zero = jnp.zeros(shape, F32)
    low = jnp.where(index >= start, value(index), zero)
    high = jnp.where(index < start, value(index + 2 * size), zero)
    return low, value(index + size), high


def wide(column, width):
    return jnp.concatenate([column] * (width // 128), axis=1)


def beams(p, off_ref, decay_ref, gy_ref, gx_ref, size):
    decay = decay_ref[p]
    for part, values in enumerate(gaussians(off_ref[p, 0], decay, size, 0)):
        gy_ref[part] = values
    for part, values in enumerate(gaussians(off_ref[p, 1], decay, size, 1)):
        gx_ref[part] = values


def row_tables(p, bins_ref, which, cos_ref, sin_ref, rows_ref, block, slots_uv):
    for k in range(slots_uv):
        at = pl.ds(pl.multiple_of(bins_ref[p, 2 * k + which] * block, block), block)
        rows_ref[(2 * k) * block : (2 * k + 1) * block, :] = cos_ref[at, :]
        rows_ref[(2 * k + 1) * block : (2 * k + 2) * block, :] = sin_ref[at, :]


def flipped_tables(p, bins_ref, cos_ref, sin_ref, flip_ref, block, slots_uv):
    for k in range(slots_uv):
        at = pl.ds(pl.multiple_of(bins_ref[p, 2 * k] * block, block), block)
        flip_ref[:, (2 * k) * block : (2 * k + 1) * block] = cos_ref[:, at]
        flip_ref[:, (2 * k + 1) * block : (2 * k + 2) * block] = sin_ref[:, at]


class Around:
    def __init__(self):
        ty, tx = lax.axis_index("ty"), lax.axis_index("tx")
        ny, nx = lax.axis_size("ty"), lax.axis_size("tx")
        self.has = (ty > 0, ty < ny - 1, tx > 0, tx < nx - 1)
        self.to = ({"ty": ty - 1}, {"ty": ty + 1}, {"tx": tx - 1}, {"tx": tx + 1})

    def greet(self):
        barrier = pltpu.get_barrier_semaphore()
        for side in range(4):

            @pl.when(self.has[side])
            def _(side=side):
                pl.semaphore_signal(barrier, inc=1, device_id=self.to[side], device_id_type=MESH)

        pl.semaphore_wait(barrier, sum(has.astype(jnp.int32) for has in self.has))


UP, DOWN, LEFT, RIGHT = 0, 1, 2, 3
BACK = (DOWN, UP, RIGHT, LEFT)


def bands(size):
    step = size // BANDS
    return [slice(i * step, (i + 1) * step) for i in range(BANDS)]


def halo_kernel(
    cosines_ref, sines_ref, own_ref,
    ul_ref, l_ref, dl_ref, ur_ref, r_ref, dr_ref, cos_out, sin_out, up_ref, down_ref,
    zero_ref, cos_ref, sin_ref, y_send, y_recv, x_send, x_recv, out_sems, zero_sem,
):
    size = own_ref.shape[0]
    length = 2 * size
    fine = FINE
    around = Around()
    pieces = bands(size)
    landing = {LEFT: (ur_ref, r_ref, dr_ref), RIGHT: (ul_ref, l_ref, dl_ref)}

    def vertical(side, i):
        target = down_ref if side == UP else up_ref
        return pltpu.make_async_remote_copy(
            src_ref=own_ref.at[pieces[i]],
            dst_ref=target.at[pieces[i]],
            send_sem=y_send.at[side, i],
            recv_sem=y_recv.at[side, i],
            device_id=around.to[side],
            device_id_type=MESH,
        )

    def beside(side):
        return pltpu.make_async_remote_copy(
            src_ref=own_ref,
            dst_ref=landing[side][1],
            send_sem=x_send.at[side - LEFT, 2 * BANDS],
            recv_sem=x_recv.at[side - LEFT, 2 * BANDS],
            device_id=around.to[side],
            device_id_type=MESH,
        )

    def corner(side, which, i):
        source = up_ref if which == 0 else down_ref
        return pltpu.make_async_remote_copy(
            src_ref=source.at[pieces[i]],
            dst_ref=landing[side][2 * which].at[pieces[i]],
            send_sem=x_send.at[side - LEFT, which * BANDS + i],
            recv_sem=x_recv.at[side - LEFT, which * BANDS + i],
            device_id=around.to[side],
            device_id_type=MESH,
        )

    zero_ref[...] = jnp.zeros_like(zero_ref)
    around.greet()
    for i in range(BANDS):
        for side in (UP, DOWN):

            @pl.when(around.has[side])
            def _(side=side, i=i):
                vertical(side, i).start()

    for side in (LEFT, RIGHT):

        @pl.when(around.has[side])
        def _(side=side):
            beside(side).start()

        @pl.when(jnp.logical_not(around.has[side]))
        def _(side=side):
            for target in landing[BACK[side]]:
                fill = pltpu.make_async_copy(zero_ref, target, zero_sem)
                fill.start()
                fill.wait()

    for side, target in ((UP, up_ref), (DOWN, down_ref)):

        @pl.when(jnp.logical_not(around.has[side]))
        def _(target=target):
            target[...] = jnp.zeros_like(target)

    def table(j, carry):
        c, s = cosines_ref[pl.ds(fine + j, 1), :], sines_ref[pl.ds(fine + j, 1), :]
        fc, fs = cosines_ref[:fine, :], sines_ref[:fine, :]
        at = pl.ds(pl.multiple_of(j * fine, fine), fine)
        cos_ref[at, :] = (fc * c - fs * s).astype(BF16)
        sin_ref[at, :] = (fs * c + fc * s).astype(BF16)
        return carry

    lax.fori_loop(0, length // fine, table, 0)

    for i in range(BANDS):
        for which, side in ((0, UP), (1, DOWN)):

            @pl.when(around.has[side])
            def _(side=side, i=i):
                vertical(BACK[side], i).wait_recv()

            for beyond in (LEFT, RIGHT):

                @pl.when(around.has[beyond])
                def _(beyond=beyond, which=which, i=i):
                    corner(beyond, which, i).start()

    cos_copy = pltpu.make_async_copy(cos_ref, cos_out, out_sems.at[0])
    sin_copy = pltpu.make_async_copy(sin_ref, sin_out, out_sems.at[1])
    cos_copy.start()
    sin_copy.start()
    for side in (UP, DOWN):

        @pl.when(around.has[side])
        def _(side=side):
            for i in range(BANDS):
                vertical(side, i).wait_send()

    for side in (LEFT, RIGHT):

        @pl.when(around.has[side])
        def _(side=side):
            beside(side).wait_send()
            beside(BACK[side]).wait_recv()
            for which in range(2):
                for i in range(BANDS):
                    corner(side, which, i).wait_send()
                    corner(BACK[side], which, i).wait_recv()

    cos_copy.wait()
    sin_copy.wait()


def early_kernel(
    count_ref, off_ref, bins_ref, decay_ref, cos_ref, sin_ref, up_ref, own_ref, down_ref,
    first_ref, gy_ref, gx_ref, rows_ref, beamed_ref,
):
    size = own_ref.shape[0]
    block = rows_ref.shape[0] // bins_ref.shape[1]
    slots_uv = bins_ref.shape[1] // 2

    def step(p, carry):
        beams(p, off_ref, decay_ref, gy_ref, gx_ref, size)
        row_tables(p, bins_ref, 0, cos_ref, sin_ref, rows_ref, block, slots_uv)
        for at in range(0, size, CHUNK):
            cols = slice(at, at + CHUNK)
            gx = gx_ref[1, 0:1, cols]
            top = wide(gy_ref[0], CHUNK) * up_ref[:, cols].astype(F32)
            top = top + wide(gy_ref[2], CHUNK) * down_ref[:, cols].astype(F32)
            beamed_ref[:size, cols] = (gx * top).astype(BF16)
            low = wide(gy_ref[1], CHUNK) * own_ref[:, cols].astype(F32)
            beamed_ref[size:, cols] = (gx * low).astype(BF16)
        for at in range(0, size, CHUNK):
            cols = slice(at, at + CHUNK)
            first_ref[p, :, cols] = jnp.dot(
                rows_ref[...], beamed_ref[:, cols], preferred_element_type=F32
            ).astype(BF16)
        return carry

    lax.fori_loop(0, count_ref[0], step, 0)


def middle_kernel(
    count_ref, off_ref, bins_ref, used_ref, decay_ref, cos_ref, sin_ref, weight_ref, early_ref,
    ul_ref, l_ref, dl_ref, ur_ref, r_ref, dr_ref,
    oul_ref, ol_ref, odl_ref, our_ref, or_ref, odr_ref, late_ref,
    gy_ref, gx_ref, rows_ref, cols_ref, flip_ref, beamed_ref, first_ref, spread_ref, acc_ref,
):
    size = l_ref.shape[0]
    block = rows_ref.shape[0] // bins_ref.shape[1]
    slots_uv = bins_ref.shape[1] // 2
    pair = 2 * block
    acc_ref[...] = jnp.zeros_like(acc_ref)

    def step(p, carry):
        beams(p, off_ref, decay_ref, gy_ref, gx_ref, size)
        row_tables(p, bins_ref, 0, cos_ref, sin_ref, rows_ref, block, slots_uv)
        row_tables(p, bins_ref, 1, cos_ref, sin_ref, cols_ref, block, slots_uv)
        flipped_tables(p, bins_ref, cos_ref, sin_ref, flip_ref, block, slots_uv)
        for at in range(0, size, CHUNK):
            cols = slice(at, at + CHUNK)
            gl = gx_ref[0, 0:1, cols]
            gr = gx_ref[2, 0:1, cols]
            gu = wide(gy_ref[0], CHUNK)
            gd = wide(gy_ref[2], CHUNK)
            left = gu * ul_ref[:, cols].astype(F32) + gd * dl_ref[:, cols].astype(F32)
            right = gu * ur_ref[:, cols].astype(F32) + gd * dr_ref[:, cols].astype(F32)
            beamed_ref[:size, cols] = (gl * left + gr * right).astype(BF16)
            low = gl * l_ref[:, cols].astype(F32) + gr * r_ref[:, cols].astype(F32)
            beamed_ref[size:, cols] = (wide(gy_ref[1], CHUNK) * low).astype(BF16)
        first_ref[:, size:] = early_ref[p]
        for at in range(0, size, CHUNK):
            cols = slice(at, at + CHUNK)
            first_ref[:, cols] = jnp.dot(
                rows_ref[...], beamed_ref[:, cols], preferred_element_type=F32
            ).astype(BF16)
        for k in range(slots_uv):
            rows = slice(k * pair, (k + 1) * pair)
            table = cols_ref[rows, :]
            both = lax.dot_general(
                first_ref[rows, :], table, (((1,), (1,)), ((), ())), preferred_element_type=F32
            )
            used = jnp.where(k < used_ref[p], 1.0, 0.0).astype(F32)
            weight = weight_ref[p, k].astype(F32) * used
            real = ((both[:block, :block] - both[block:, block:]) * weight).astype(BF16)
            turned = ((both[:block, block:] + both[block:, :block]) * weight).astype(BF16)
            scaled = jnp.concatenate(
                [
                    jnp.concatenate([real, turned], axis=1),
                    jnp.concatenate([turned, -real], axis=1),
                ],
                axis=0,
            )
            spread_ref[rows, :] = jnp.dot(scaled, table, preferred_element_type=F32).astype(BF16)
        late_ref[p] = spread_ref[:, size:]
        for at in range(0, size, CHUNK):
            cols = slice(at, at + CHUNK)
            gl = gx_ref[0, 0:1, cols]
            gr = gx_ref[2, 0:1, cols]
            top = jnp.dot(flip_ref[:size, :], spread_ref[:, cols], preferred_element_type=F32)
            up = wide(gy_ref[0], CHUNK) * top
            down = wide(gy_ref[2], CHUNK) * top
            acc_ref[0, :, cols] += gl * up
            acc_ref[2, :, cols] += gl * down
            acc_ref[3, :, cols] += gr * up
            acc_ref[5, :, cols] += gr * down
            low = jnp.dot(flip_ref[size:, :], spread_ref[:, cols], preferred_element_type=F32)
            low = wide(gy_ref[1], CHUNK) * low
            acc_ref[1, :, cols] += gl * low
            acc_ref[4, :, cols] += gr * low
        return carry

    def idle(p, carry):
        late_ref[p] = jnp.zeros(late_ref.shape[1:], BF16)
        return carry

    lax.fori_loop(0, count_ref[0], step, 0)
    lax.fori_loop(count_ref[0], late_ref.shape[0], idle, 0)
    for part, out_ref in enumerate((oul_ref, ol_ref, odl_ref, our_ref, or_ref, odr_ref)):
        out_ref[...] = acc_ref[part].astype(BF16)


def late_kernel(
    count_ref, off_ref, bins_ref, decay_ref, cos_ref, sin_ref, late_ref,
    up_ref, own_ref, down_ref, gy_ref, gx_ref, flip_ref,
):
    size = own_ref.shape[0]
    block = flip_ref.shape[1] // bins_ref.shape[1]
    slots_uv = bins_ref.shape[1] // 2
    for out_ref in (up_ref, own_ref, down_ref):
        out_ref[...] = jnp.zeros_like(out_ref)

    def step(p, carry):
        beams(p, off_ref, decay_ref, gy_ref, gx_ref, size)
        flipped_tables(p, bins_ref, cos_ref, sin_ref, flip_ref, block, slots_uv)
        for at in range(0, size, CHUNK):
            cols = slice(at, at + CHUNK)
            gx = gx_ref[1, 0:1, cols]
            part = late_ref[p, :, cols]
            top = gx * jnp.dot(flip_ref[:size, :], part, preferred_element_type=F32)
            up_ref[:, cols] += wide(gy_ref[0], CHUNK) * top
            down_ref[:, cols] += wide(gy_ref[2], CHUNK) * top
            low = gx * jnp.dot(flip_ref[size:, :], part, preferred_element_type=F32)
            own_ref[:, cols] += wide(gy_ref[1], CHUNK) * low
        return carry

    lax.fori_loop(0, count_ref[0], step, 0)


def sum_kernel(
    ul_ref, l_ref, dl_ref, ur_ref, r_ref, dr_ref, up_ref, mid_ref, down_ref,
    own_ref, above_ref, below_ref, got_ref, going_ref,
    y_send, y_recv, x_send, x_recv,
):
    size = own_ref.shape[0]
    around = Around()
    pieces = bands(size)
    leaving = {LEFT: (ul_ref, l_ref, dl_ref), RIGHT: (ur_ref, r_ref, dr_ref)}

    def corner(side, which, i):
        return pltpu.make_async_remote_copy(
            src_ref=leaving[side][2 * which].at[pieces[i]],
            dst_ref=got_ref.at[side - LEFT, 2 * which, pieces[i]],
            send_sem=x_send.at[side - LEFT, which * BANDS + i],
            recv_sem=x_recv.at[side - LEFT, which * BANDS + i],
            device_id=around.to[side],
            device_id_type=MESH,
        )

    def beside(side):
        return pltpu.make_async_remote_copy(
            src_ref=leaving[side][1],
            dst_ref=got_ref.at[side - LEFT, 1],
            send_sem=x_send.at[side - LEFT, 2 * BANDS],
            recv_sem=x_recv.at[side - LEFT, 2 * BANDS],
            device_id=around.to[side],
            device_id_type=MESH,
        )

    def vertical(side, i):
        target = below_ref if side == UP else above_ref
        return pltpu.make_async_remote_copy(
            src_ref=going_ref.at[side, pieces[i]],
            dst_ref=target.at[pieces[i]],
            send_sem=y_send.at[side, i],
            recv_sem=y_recv.at[side, i],
            device_id=around.to[side],
            device_id_type=MESH,
        )

    around.greet()
    for i in range(BANDS):
        for which in range(2):
            for side in (LEFT, RIGHT):

                @pl.when(around.has[side])
                def _(side=side, which=which, i=i):
                    corner(side, which, i).start()

    for side in (LEFT, RIGHT):

        @pl.when(around.has[side])
        def _(side=side):
            beside(side).start()

        @pl.when(jnp.logical_not(around.has[side]))
        def _(side=side):
            got_ref[BACK[side] - LEFT] = jnp.zeros(got_ref.shape[1:], BF16)

    for side, target in ((UP, above_ref), (DOWN, below_ref)):

        @pl.when(jnp.logical_not(around.has[side]))
        def _(target=target):
            target[...] = jnp.zeros_like(target)

    for i in range(BANDS):
        for which, part_ref in ((0, up_ref), (1, down_ref)):
            for side in (LEFT, RIGHT):

                @pl.when(around.has[side])
                def _(side=side, which=which, i=i):
                    corner(BACK[side], which, i).wait_recv()

            total = part_ref[pieces[i], :]
            for back in range(2):
                total = total + got_ref[back, 2 * which, pieces[i], :].astype(F32)
            going_ref[which, pieces[i], :] = total.astype(BF16)
        for side in (UP, DOWN):

            @pl.when(around.has[side])
            def _(side=side, i=i):
                vertical(side, i).start()

    for side in (LEFT, RIGHT):

        @pl.when(around.has[side])
        def _(side=side):
            beside(BACK[side]).wait_recv()

    own_ref[...] = mid_ref[...] + got_ref[0, 1].astype(F32) + got_ref[1, 1].astype(F32)
    for side in (LEFT, RIGHT):

        @pl.when(around.has[side])
        def _(side=side):
            beside(side).wait_send()
            for which in range(2):
                for i in range(BANDS):
                    corner(side, which, i).wait_send()

    for side in (UP, DOWN):

        @pl.when(around.has[side])
        def _(side=side):
            for i in range(BANDS):
                vertical(side, i).wait_send()
                vertical(BACK[side], i).wait_recv()


def remote_call(kernel, ident, scalars, anys, vectors, outs, spaces, scratch):
    return pl.pallas_call(
        kernel,
        out_shape=outs,
        in_specs=[pl.BlockSpec(memory_space=pltpu.SMEM)] * len(scalars)
        + [pl.BlockSpec(memory_space=pl.ANY)] * len(anys)
        + [pl.BlockSpec(memory_space=pltpu.VMEM)] * len(vectors),
        out_specs=tuple(pl.BlockSpec(memory_space=space) for space in spaces),
        scratch_shapes=scratch,
        compiler_params=pltpu.CompilerParams(
            vmem_limit_bytes=56 * 1024 * 1024, collective_id=ident, has_side_effects=True
        ),
    )(*scalars, *anys, *vectors)


def local_call(kernel, scalars, vectors, outs, scratch, flops):
    return pl.pallas_call(
        kernel,
        out_shape=outs,
        in_specs=[pl.BlockSpec(memory_space=pltpu.SMEM)] * len(scalars)
        + [pl.BlockSpec(memory_space=pltpu.VMEM)] * len(vectors),
        out_specs=jax.tree.map(lambda _: pl.BlockSpec(memory_space=pltpu.VMEM), outs),
        scratch_shapes=scratch,
        compiler_params=pltpu.CompilerParams(vmem_limit_bytes=56 * 1024 * 1024),
        cost_estimate=pl.CostEstimate(flops=flops, bytes_accessed=8 << 20, transcendentals=0),
    )(*scalars, *vectors)


def shards(sky, point_count, point_offset, beam_width, uv_bins, uv_count, uv_weight):
    size = sky.shape[0]
    length = 2 * size
    slots, slots_uv, block = uv_weight.shape[2], uv_weight.shape[3], uv_weight.shape[4]
    depth = 2 * slots_uv * block
    cosines, sines = small_tables(length, FINE)
    count = point_count.reshape(1)
    offset = point_offset.reshape(slots, 2)
    bins = jnp.clip(uv_bins.reshape(slots, 2 * slots_uv), 0, length // block - 1)
    used = uv_count.reshape(slots)
    width = beam_width.reshape(slots).astype(F32)
    decay = 1.0 / (2.0 * width * width)
    weight = uv_weight.reshape(slots, slots_uv, block, block)

    gy = pltpu.VMEM((3, size, 128), F32)
    gx = pltpu.VMEM((3, 8, size), F32)
    rows = pltpu.VMEM((depth, length), BF16)
    flip = pltpu.VMEM((length, depth), BF16)
    beamed = pltpu.VMEM((length, size), BF16)
    half = jax.ShapeDtypeStruct((slots, depth, size), BF16)
    sent = jax.ShapeDtypeStruct((size, size), BF16)
    kept = jax.ShapeDtypeStruct((size, size), F32)
    flops = 2 * slots * depth * length * size

    dma = pltpu.SemaphoreType.DMA
    tile = pltpu.VMEM((size, size), BF16)
    table = pltpu.VMEM((length, length), BF16)
    sems = [dma((2, BANDS))] * 2 + [dma((2, 2 * BANDS + 1))] * 2
    full = jax.ShapeDtypeStruct((length, length), BF16)
    up_left, left, down_left, up_right, right, down_right, cos, sin, up, down = remote_call(
        halo_kernel,
        0,
        (),
        (),
        (cosines, sines, sky),
        (sent,) * 6 + (full, full, sent, sent),
        (pl.ANY,) * 8 + (pltpu.VMEM,) * 2,
        [tile, table, table] + sems + [dma((2,)), dma],
    )
    early = local_call(
        early_kernel,
        (count, offset, bins, decay),
        (cos, sin, up, sky, down),
        half,
        [gy, gx, rows, beamed],
        flops,
    )
    to_ul, to_l, to_dl, to_ur, to_r, to_dr, late = local_call(
        middle_kernel,
        (count, offset, bins, used, decay),
        (cos, sin, weight, early, up_left, left, down_left, up_right, right, down_right),
        (sent,) * 6 + (half,),
        [
            gy, gx, rows, rows, flip, beamed,
            pltpu.VMEM((depth, length), BF16),
            pltpu.VMEM((depth, length), BF16),
            pltpu.VMEM((6, size, size), F32),
        ],
        3 * flops,
    )
    to_up, own, to_down = local_call(
        late_kernel,
        (count, offset, bins, decay),
        (cos, sin, late),
        (kept,) * 3,
        [gy, gx, flip],
        flops,
    )
    own, above, below = remote_call(
        sum_kernel,
        1,
        (),
        (to_ul, to_l, to_dl, to_ur, to_r, to_dr),
        (to_up, own, to_down),
        (kept, sent, sent),
        (pltpu.VMEM,) * 3,
        [pltpu.VMEM((2, 3, size, size), BF16), pltpu.VMEM((2, size, size), BF16)] + sems,
    )
    return own + above.astype(F32) + below.astype(F32)


def solution(mesh):
    in_specs = (
        P("ty", "tx"),
        P("ty", "tx"),
        P("ty", "tx", None, None),
        P("ty", "tx", None),
        P("ty", "tx", None, None, None),
        P("ty", "tx", None),
        P("ty", "tx", None, None, None, None),
    )
    out_specs = P("ty", "tx")
    return jax.shard_map(shards, mesh=mesh, in_specs=in_specs, out_specs=out_specs, check_vma=False)
```
